32 devices in a mesh: spin: 2 (over x), band: 16 (over z, y, core).
Axes of the slice: x: 2, y: 2, z: 4, core: 2. Of those that a mesh axis runs over, the one named last changes fastest.
Arguments:
- orbitals: bfloat16 [32, 262144], P(('spin', 'band')), parts along dimension 0, may hold values from -6 to 6
- trial: bfloat16 [32, 262144], P(('spin', 'band')), parts along dimension 0, may hold values from -6 to 6
- occupations: int32 [32], P(('spin', 'band')), parts along dimension 0, may hold values 0 or 1
Outputs:
- exchange: bfloat16 [32, 262144], P(('spin', 'band')), parts along dimension 0
- projected: bfloat16 [32, 262144], P('spin', 'band'), parts along dimension 0
The draws below stay inside these ranges and needn't reach their ends.
There are 2 independent parts, one for each index of `spin`. The reference program is written for one: setup_inputs(seed, part) draws one part's arguments, and reference() takes and returns one part's arrays. A program takes and returns all parts, laid end to end along the dimension named above; each array names one. Nothing has to cross between parts.
All inputs are finite; a program needn't handle non-finite values. No bound on the sum of `occupations` on one device may be relied on, other than what follows from the above.
Results may differ from the reference program's by a relative error of at most 0.018.
Values may be sent and summed in bfloat16 or wider, within the bound.
A program may use at most 64 MiB of HBM per device.

```python
import math
import jax
import jax.numpy as jnp
from jax import lax

NG = 64
ORB_DEV = 1
SHIFTS = 1
G = 262144
ORBITALS = 16
N_BAND = 16


def touch_ends(values, stream_key, smallest, high):
    longest = values.shape.index(max(values.shape))
    spots = []
    for shift in (0, 1):
        where = [jax.random.randint(jax.random.fold_in(stream_key, axis), (), 0, length) for axis, length in enumerate(values.shape)]
        where[longest] = (where[longest] + shift) % values.shape[longest]
        spots.append(tuple(where))
    return values.at[spots[0]].set(smallest).at[spots[1]].set(high)


def block_levels(rng, shape, shards, smallest, top_value):
    level, own = 1.0, jax.random.fold_in(rng, 6)
    for position, blocks in shards:
        draws = jnp.exp(jax.random.uniform(jax.random.fold_in(own, position), (blocks,), jnp.float32, smallest / len(shards), top_value / len(shards)))
        level = level * jnp.repeat(draws, shape[position] // blocks).reshape([-1 if axis == position else 1 for axis in range(len(shape))])
    return level


def bell_draw(stream_key, shape, scale, reach, pieces=(), held_as=jnp.bfloat16):
    array = jax.random.normal(stream_key, shape, jnp.float32) * scale
    if len(pieces) > 0:
        array = block_levels(stream_key, shape, pieces, -0.22, 0.18) * array
    return jnp.clip(array, min=-reach, max=reach).astype(held_as)


def setup_inputs(seed: int = 0, part: int = 0) -> dict:
    keys = jax.random.split(jax.random.key(seed), 4)
    own_keys = jax.random.split(jax.random.fold_in(keys[3], part), 4)
    return {
        "orbitals": bell_draw(own_keys[0], (ORBITALS, G), 1.0, 6.0, ((0, 16),)),
        "trial": bell_draw(own_keys[1], (ORBITALS, G), 1.0, 6.0, ((0, 16),)),
        "occupations": touch_ends((jax.random.randint(own_keys[2], (ORBITALS,), 0, 4) < 3).astype(jnp.int32), jax.random.fold_in(own_keys[2], 1), 0, 1),
    }


FRACTION = 0.25
OMEGA = 1.0

def cas_table(extent):
    indices = jnp.arange(extent, dtype=jnp.int32)
    products = indices[:, None] * indices[None, :] % extent
    phases = products.astype(jnp.float32) * (2.0 * math.pi / extent)
    return (jnp.cos(phases) + jnp.sin(phases)).astype(jnp.bfloat16)

def screened_kernel(extent):
    modes = jnp.arange(extent, dtype=jnp.int32)
    modes = jnp.where(2 * modes < extent, modes, modes - extent)
    wavenum = modes.astype(jnp.float32) * (2.0 * math.pi / extent)
    squares = wavenum * wavenum
    norm_sq = squares[:, None, None] + squares[None, :, None] + squares[None, None, :]
    bounded = jnp.where(norm_sq > 0, norm_sq, 1.0)
    screened = jnp.where(norm_sq > 0, 4.0 * math.pi / bounded * (1.0 - jnp.exp(-bounded / (4.0 * OMEGA * OMEGA))), math.pi / (OMEGA * OMEGA))
    return (screened / extent ** 3).reshape(-1)

def sweep(values, pattern, table):
    rounded = lax.optimization_barrier(values)
    return jnp.einsum(pattern, table.astype(jnp.float32), rounded.astype(jnp.float32), precision=lax.Precision.HIGHEST)

def screened_potential(density, table, kernel, extent):
    number = density.shape[0]
    values = density.reshape(number, extent, extent, extent)
    patterns = ('ga,pabc->pgbc', 'gb,pabc->pagc', 'gc,pabc->pabg')
    for pattern in patterns:
        values = sweep(values, pattern, table).astype(jnp.bfloat16)
    values = lax.optimization_barrier(values)
    values = (values.astype(jnp.float32) * kernel.reshape(extent, extent, extent)).astype(jnp.bfloat16)
    for ordinal, pattern in enumerate(patterns):
        values = sweep(values, pattern, table)
        if ordinal < 2:
            values = values.astype(jnp.bfloat16)
    return values.reshape(number, -1)

def reference(orbitals, trial, occupations):
    table = cas_table(NG)
    kernel = screened_kernel(NG)
    blocks = orbitals.reshape(N_BAND, ORB_DEV, G)
    fills = occupations.astype(jnp.float32).reshape(N_BAND, ORB_DEV)

    def one_block(block_index):
        own = lax.dynamic_index_in_dim(blocks, block_index, 0, keepdims=False)
        accumulated = jnp.zeros((ORB_DEV, G), jnp.float32)
        for offset in range(-SHIFTS, SHIFTS + 1):
            partner = ((block_index - offset) % N_BAND).astype(jnp.int32)
            visitors = lax.dynamic_index_in_dim(blocks, partner, 0, keepdims=False)
            partner_fill = lax.dynamic_index_in_dim(fills, partner, 0, keepdims=False)
            density = (own[:, None, :].astype(jnp.float32) * visitors[None, :, :].astype(jnp.float32)).astype(jnp.bfloat16)
            potential = screened_potential(density.reshape(ORB_DEV * ORB_DEV, G), table, kernel, NG).reshape(ORB_DEV, ORB_DEV, G)
            accumulated = accumulated + jnp.einsum('ijg,j,jg->ig', potential, partner_fill, visitors.astype(jnp.float32), precision=lax.Precision.HIGHEST)
        return (-FRACTION * accumulated).astype(jnp.bfloat16)
    exchange = lax.map(one_block, jnp.arange(N_BAND, dtype=jnp.int32)).reshape(ORBITALS, G)
    intersection = lax.dot_general(exchange, trial, (((1,), (1,)), ((), ())), preferred_element_type=jnp.float32) / math.sqrt(G)
    intersection_low = intersection.astype(jnp.bfloat16)
    projected = -(lax.dot_general(intersection_low, exchange, (((0,), (0,)), ((), ())), preferred_element_type=jnp.float32) / math.sqrt(ORBITALS))
    return (exchange, projected.astype(jnp.bfloat16))
```

```python
import functools
import math

import jax
import jax.numpy as jnp
from jax import lax
from jax.experimental import pallas as pl
from jax.experimental.pallas import tpu as pltpu
from jax.sharding import PartitionSpec as P

NG = 64
FRACTION = 0.25
OMEGA = 1.0
MESH = pl.DeviceIdType.MESH


def passed_along(value, axis, steps):
    count = lax.axis_size(axis)
    pairs = [(source, (source + steps) % count) for source in range(count)]
    return lax.ppermute(value, axis, pairs)


def cas_table(extent):
    indices = jnp.arange(extent, dtype=jnp.int32)
    products = indices[:, None] * indices[None, :] % extent
    phases = products.astype(jnp.float32) * (2.0 * math.pi / extent)
    return (jnp.cos(phases) + jnp.sin(phases)).astype(jnp.bfloat16)


def screened_kernel(extent):
    modes = jnp.arange(extent, dtype=jnp.int32)
    modes = jnp.where(2 * modes < extent, modes, modes - extent)
    wavenum = modes.astype(jnp.float32) * (2.0 * math.pi / extent)
    squares = wavenum * wavenum
    norm_sq = squares[:, None, None] + squares[None, :, None] + squares[None, None, :]
    bounded = jnp.where(norm_sq > 0, norm_sq, 1.0)
    screened = jnp.where(
        norm_sq > 0,
        4.0 * math.pi / bounded * (1.0 - jnp.exp(-bounded / (4.0 * OMEGA * OMEGA))),
        math.pi / (OMEGA * OMEGA),
    )
    return screened / extent**3


def screened_potential(values, table, kernel):
    patterns = ("ga,abc->gbc", "gb,abc->agc", "gc,abc->abg")
    for pattern in patterns:
        values = jnp.einsum(pattern, table, values, preferred_element_type=jnp.float32).astype(
            jnp.bfloat16
        )
    values = (values.astype(jnp.float32) * kernel).astype(jnp.bfloat16)
    for ordinal, pattern in enumerate(patterns):
        values = jnp.einsum(pattern, table, values, preferred_element_type=jnp.float32)
        if ordinal < 2:
            values = values.astype(jnp.bfloat16)
    return values


def greet(count, me):
    barrier = pltpu.get_barrier_semaphore()

    @pl.loop(1, count)
    def _(step):
        peer = lax.rem(me + step, count)
        pl.semaphore_signal(barrier, inc=1, device_id={"band": peer}, device_id_type=MESH)

    pl.semaphore_wait(barrier, count - 1)


def slabs_body(count, arrays, *refs):
    ins, outs = refs[:arrays], refs[arrays : 2 * arrays]
    send_sem, recv_sem, own_sem = refs[2 * arrays :]
    me = lax.axis_index("band")
    greet(count, me)

    def remote(which, peer, slot):
        return pltpu.make_async_remote_copy(
            src_ref=ins[which].at[peer],
            dst_ref=outs[which].at[slot],
            send_sem=send_sem.at[which, peer],
            recv_sem=recv_sem.at[which, slot],
            device_id={"band": peer},
            device_id_type=MESH,
        )

    def own(which):
        return pltpu.make_async_copy(ins[which].at[me], outs[which].at[me], own_sem.at[which])

    for which in range(arrays):

        @pl.loop(1, count)
        def _(step):
            remote(which, lax.rem(me + step, count), me).start()

        own(which).start()
    for which in range(arrays):
        own(which).wait()

        @pl.loop(1, count)
        def _(step):
            remote(which, lax.rem(me + step, count), me).wait_send()

        @pl.loop(1, count)
        def _(step):
            peer = lax.rem(me + count - step, count)
            remote(which, peer, peer).wait_recv()


def to_slabs(arrays, collective_id):
    count = lax.axis_size("band")
    number = len(arrays)
    shape = arrays[0].shape
    size = math.prod(shape)
    return pl.pallas_call(
        functools.partial(slabs_body, count, number),
        out_shape=[jax.ShapeDtypeStruct(shape, a.dtype) for a in arrays],
        in_specs=[pl.BlockSpec(memory_space=pltpu.VMEM)] * number,
        out_specs=[pl.BlockSpec(memory_space=pltpu.VMEM)] * number,
        scratch_shapes=[
            pltpu.SemaphoreType.DMA((number, count)),
            pltpu.SemaphoreType.DMA((number, count)),
            pltpu.SemaphoreType.DMA((number,)),
        ],
        cost_estimate=pl.CostEstimate(
            flops=0, bytes_accessed=size * 40 * number, transcendentals=0
        ),
        compiler_params=pltpu.CompilerParams(
            collective_id=collective_id, has_side_effects=True
        ),
        name="to_slabs",
    )(*arrays)


def summed_body(count, part_ref, total_ref, parts, send_sem, recv_sem):
    me = lax.axis_index("band")
    greet(count, me)

    def remote(peer, slot):
        return pltpu.make_async_remote_copy(
            src_ref=part_ref,
            dst_ref=parts.at[slot],
            send_sem=send_sem.at[peer],
            recv_sem=recv_sem.at[slot],
            device_id={"band": peer},
            device_id_type=MESH,
        )

    @pl.loop(1, count)
    def _(step):
        remote(lax.rem(me + step, count), me).start()

    parts[pl.ds(me, 1)] = part_ref[...][None]

    @pl.loop(1, count)
    def _(step):
        remote(lax.rem(me + step, count), me).wait_send()

    @pl.loop(1, count)
    def _(step):
        peer = lax.rem(me + count - step, count)
        remote(peer, peer).wait_recv()

    total_ref[...] = jnp.sum(parts[...], axis=0)


def summed(part, collective_id):
    count = lax.axis_size("band")
    return pl.pallas_call(
        functools.partial(summed_body, count),
        out_shape=jax.ShapeDtypeStruct(part.shape, part.dtype),
        in_specs=[pl.BlockSpec(memory_space=pltpu.VMEM)],
        out_specs=pl.BlockSpec(memory_space=pltpu.VMEM),
        scratch_shapes=[
            pltpu.VMEM((count,) + part.shape, part.dtype),
            pltpu.SemaphoreType.DMA((count,)),
            pltpu.SemaphoreType.DMA((count,)),
        ],
        compiler_params=pltpu.CompilerParams(
            collective_id=collective_id, has_side_effects=True
        ),
        name="summed",
    )(part)


def local(orbitals, trial, occupations):
    count = lax.axis_size("band")
    cells = orbitals.shape[1]
    extent = NG
    table = cas_table(extent)
    kernel = screened_kernel(extent)
    cube = (extent, extent, extent)
    fill = occupations.astype(jnp.bfloat16)

    visitor, visitor_fill = passed_along((orbitals, fill), "band", 1)
    own = orbitals.reshape(cube).astype(jnp.float32)
    own_weighted = own * fill[0].astype(jnp.float32)
    own_potential = screened_potential((own * own).astype(jnp.bfloat16), table, kernel)
    accumulated = own_potential * own_weighted

    other = visitor.reshape(cube).astype(jnp.float32)
    potential = screened_potential((own * other).astype(jnp.bfloat16), table, kernel)
    carried = passed_along((potential * own_weighted).astype(jnp.bfloat16), "band", -1)
    accumulated = accumulated + potential * (other * visitor_fill[0].astype(jnp.float32))
    accumulated = accumulated + carried.astype(jnp.float32)
    exchange = (-FRACTION * accumulated).astype(jnp.bfloat16).reshape(1, cells)

    slab = (count, cells // count // 128, 128)
    grid_exchange, grid_trial = to_slabs((exchange.reshape(slab), trial.reshape(slab)), 1)
    grid_exchange = grid_exchange.reshape(count, -1)
    grid_trial = grid_trial.reshape(count, -1)
    part = lax.dot_general(
        grid_exchange, grid_trial, (((1,), (1,)), ((), ())), preferred_element_type=jnp.float32
    )
    intersection_low = (summed(part, 2) / math.sqrt(cells)).astype(jnp.bfloat16)
    projected = -(
        lax.dot_general(
            intersection_low,
            grid_exchange,
            (((0,), (0,)), ((), ())),
            preferred_element_type=jnp.float32,
        )
        / math.sqrt(count)
    )
    return (exchange, projected.astype(jnp.bfloat16))


def solution(mesh):
    return jax.shard_map(
        local,
        mesh=mesh,
        in_specs=(P(("spin", "band"), None), P(("spin", "band"), None), P(("spin", "band"))),
        out_specs=(P(("spin", "band"), None), P("spin", "band")),
        check_vma=False,
    )
```

```python
import functools
import math

import jax
import jax.numpy as jnp
from jax import lax
from jax.experimental import pallas as pl
from jax.experimental.pallas import tpu as pltpu
from jax.sharding import PartitionSpec as P

NG = 64
FRACTION = 0.25
OMEGA = 1.0
CHUNK = 2048
MESH = pl.DeviceIdType.MESH


def passed_along(value, axis, steps):
    count = lax.axis_size(axis)
    pairs = [(source, (source + steps) % count) for source in range(count)]
    return lax.ppermute(value, axis, pairs)


def cas_table(extent):
    indices = jnp.arange(extent, dtype=jnp.int32)
    products = indices[:, None] * indices[None, :] % extent
    phases = products.astype(jnp.float32) * (2.0 * math.pi / extent)
    return (jnp.cos(phases) + jnp.sin(phases)).astype(jnp.bfloat16)


def screened_kernel(extent):
    modes = jnp.arange(extent, dtype=jnp.int32)
    modes = jnp.where(2 * modes < extent, modes, modes - extent)
    wavenum = modes.astype(jnp.float32) * (2.0 * math.pi / extent)
    squares = wavenum * wavenum
    norm_sq = squares[:, None, None] + squares[None, :, None] + squares[None, None, :]
    bounded = jnp.where(norm_sq > 0, norm_sq, 1.0)
    screened = jnp.where(
        norm_sq > 0,
        4.0 * math.pi / bounded * (1.0 - jnp.exp(-bounded / (4.0 * OMEGA * OMEGA))),
        math.pi / (OMEGA * OMEGA),
    )
    return screened / extent**3


def screened_potential(values, table, kernel):
    patterns = ("ga,abc->gbc", "gb,abc->agc", "gc,abc->abg")
    for pattern in patterns:
        values = jnp.einsum(pattern, table, values, preferred_element_type=jnp.float32).astype(
            jnp.bfloat16
        )
    values = (values.astype(jnp.float32) * kernel).astype(jnp.bfloat16)
    for ordinal, pattern in enumerate(patterns):
        values = jnp.einsum(pattern, table, values, preferred_element_type=jnp.float32)
        if ordinal < 2:
            values = values.astype(jnp.bfloat16)
    return values


def greet(count, me):
    barrier = pltpu.get_barrier_semaphore()

    @pl.loop(1, count)
    def _(step):
        peer = lax.rem(me + step, count)
        pl.semaphore_signal(barrier, inc=1, device_id={"band": peer}, device_id_type=MESH)

    pl.semaphore_wait(barrier, count - 1)


def slabs_body(count, arrays, *refs):
    ins, outs = refs[:arrays], refs[arrays : 2 * arrays]
    send_sem, recv_sem, own_sem = refs[2 * arrays :]
    me = lax.axis_index("band")
    greet(count, me)

    def remote(which, peer, slot):
        return pltpu.make_async_remote_copy(
            src_ref=ins[which].at[peer],
            dst_ref=outs[which].at[slot],
            send_sem=send_sem.at[which, peer],
            recv_sem=recv_sem.at[which, slot],
            device_id={"band": peer},
            device_id_type=MESH,
        )

    def own(which):
        return pltpu.make_async_copy(ins[which].at[me], outs[which].at[me], own_sem.at[which])

    for which in range(arrays):

        @pl.loop(1, count)
        def _(step):
            remote(which, lax.rem(me + step, count), me).start()

        own(which).start()
    for which in range(arrays):
        own(which).wait()

        @pl.loop(1, count)
        def _(step):
            remote(which, lax.rem(me + step, count), me).wait_send()

        @pl.loop(1, count)
        def _(step):
            peer = lax.rem(me + count - step, count)
            remote(which, peer, peer).wait_recv()


def to_slabs(arrays, collective_id):
    count = lax.axis_size("band")
    number = len(arrays)
    shape = arrays[0].shape
    size = math.prod(shape)
    return pl.pallas_call(
        functools.partial(slabs_body, count, number),
        out_shape=[jax.ShapeDtypeStruct(shape, a.dtype) for a in arrays],
        in_specs=[pl.BlockSpec(memory_space=pltpu.VMEM)] * number,
        out_specs=[pl.BlockSpec(memory_space=pltpu.VMEM)] * number,
        scratch_shapes=[
            pltpu.SemaphoreType.DMA((number, count)),
            pltpu.SemaphoreType.DMA((number, count)),
            pltpu.SemaphoreType.DMA((number,)),
        ],
        cost_estimate=pl.CostEstimate(
            flops=0, bytes_accessed=size * 40 * number, transcendentals=0
        ),
        compiler_params=pltpu.CompilerParams(
            collective_id=collective_id, has_side_effects=True
        ),
        name="to_slabs",
    )(*arrays)


def summed_body(count, part_ref, total_ref, parts, send_sem, recv_sem):
    me = lax.axis_index("band")
    greet(count, me)

    def remote(peer, slot):
        return pltpu.make_async_remote_copy(
            src_ref=part_ref,
            dst_ref=parts.at[slot],
            send_sem=send_sem.at[peer],
            recv_sem=recv_sem.at[slot],
            device_id={"band": peer},
            device_id_type=MESH,
        )

    @pl.loop(1, count)
    def _(step):
        remote(lax.rem(me + step, count), me).start()

    parts[pl.ds(me, 1)] = part_ref[...][None]

    @pl.loop(1, count)
    def _(step):
        remote(lax.rem(me + step, count), me).wait_send()

    @pl.loop(1, count)
    def _(step):
        peer = lax.rem(me + count - step, count)
        remote(peer, peer).wait_recv()

    total_ref[...] = jnp.sum(parts[...], axis=0)


def summed(part, collective_id):
    count = lax.axis_size("band")
    return pl.pallas_call(
        functools.partial(summed_body, count),
        out_shape=jax.ShapeDtypeStruct(part.shape, part.dtype),
        in_specs=[pl.BlockSpec(memory_space=pltpu.VMEM)],
        out_specs=pl.BlockSpec(memory_space=pltpu.VMEM),
        scratch_shapes=[
            pltpu.VMEM((count,) + part.shape, part.dtype),
            pltpu.SemaphoreType.DMA((count,)),
            pltpu.SemaphoreType.DMA((count,)),
        ],
        compiler_params=pltpu.CompilerParams(
            collective_id=collective_id, has_side_effects=True
        ),
        name="summed",
    )(part)


def rows_body(chunk, *refs):
    half = len(refs) // 2
    for line, rows in zip(refs[:half], refs[half:]):

        @pl.loop(0, line.shape[1] // chunk, unroll=4)
        def _(step):
            cut = pl.ds(pl.multiple_of(step * chunk, chunk), chunk)
            out = pl.ds(pl.multiple_of(step * (chunk // 128), chunk // 128), chunk // 128)
            wide = line[:, cut].astype(jnp.float32).reshape(chunk // 128, 128)
            rows[out, :] = wide.astype(rows.dtype)


def as_rows(*lines):
    number = len(lines)
    cells = lines[0].shape[1]
    return pl.pallas_call(
        functools.partial(rows_body, CHUNK),
        out_shape=[jax.ShapeDtypeStruct((cells // 128, 128), a.dtype) for a in lines],
        in_specs=[pl.BlockSpec(memory_space=pltpu.VMEM)] * number,
        out_specs=[pl.BlockSpec(memory_space=pltpu.VMEM)] * number,
        cost_estimate=pl.CostEstimate(
            flops=0, bytes_accessed=cells * 16 * number, transcendentals=0
        ),
        name="as_rows",
    )(*lines)


def local(orbitals, trial, occupations):
    count = lax.axis_size("band")
    cells = orbitals.shape[1]
    extent = NG
    table = cas_table(extent)
    kernel = screened_kernel(extent)
    cube = (extent, extent, extent)
    fill = occupations.astype(jnp.bfloat16)

    (lined,) = as_rows(orbitals)
    (trial_rows,) = as_rows(trial)
    visitor, visitor_fill = passed_along((lined, fill), "band", 1)
    own = lined.reshape(cube).astype(jnp.float32)
    own_weighted = own * fill[0].astype(jnp.float32)
    own_potential = screened_potential((own * own).astype(jnp.bfloat16), table, kernel)
    accumulated = own_potential * own_weighted

    other = visitor.reshape(cube).astype(jnp.float32)
    potential = screened_potential((own * other).astype(jnp.bfloat16), table, kernel)
    carried = passed_along((potential * own_weighted).astype(jnp.bfloat16), "band", -1)
    accumulated = accumulated + potential * (other * visitor_fill[0].astype(jnp.float32))
    accumulated = accumulated + carried.astype(jnp.float32)
    exchange = (-FRACTION * accumulated).astype(jnp.bfloat16).reshape(1, cells)

    slab = (count, cells // count // 128, 128)
    grid_exchange, grid_trial = to_slabs((exchange.reshape(slab), trial_rows.reshape(slab)), 1)
    grid_exchange = grid_exchange.reshape(count, -1)
    grid_trial = grid_trial.reshape(count, -1)
    part = lax.dot_general(
        grid_exchange, grid_trial, (((1,), (1,)), ((), ())), preferred_element_type=jnp.float32
    )
    intersection_low = (summed(part, 2) / math.sqrt(cells)).astype(jnp.bfloat16)
    projected = -(
        lax.dot_general(
            intersection_low,
            grid_exchange,
            (((0,), (0,)), ((), ())),
            preferred_element_type=jnp.float32,
        )
        / math.sqrt(count)
    )
    return (exchange, projected.astype(jnp.bfloat16))


def solution(mesh):
    return jax.shard_map(
        local,
        mesh=mesh,
        in_specs=(P(("spin", "band"), None), P(("spin", "band"), None), P(("spin", "band"))),
        out_specs=(P(("spin", "band"), None), P("spin", "band")),
        check_vma=False,
    )
```

```python
import functools
import math

import jax
import jax.numpy as jnp
from jax import lax
from jax.experimental import pallas as pl
from jax.experimental.pallas import tpu as pltpu
from jax.sharding import PartitionSpec as P

NG = 64
FRACTION = 0.25
OMEGA = 1.0
CHUNK = 2048
MESH = pl.DeviceIdType.MESH


def passed_along(value, axis, steps):
    count = lax.axis_size(axis)
    pairs = [(source, (source + steps) % count) for source in range(count)]
    return lax.ppermute(value, axis, pairs)


def cas_table(extent):
    indices = jnp.arange(extent, dtype=jnp.int32)
    products = indices[:, None] * indices[None, :] % extent
    phases = products.astype(jnp.float32) * (2.0 * math.pi / extent)
    return (jnp.cos(phases) + jnp.sin(phases)).astype(jnp.bfloat16)


def screened_kernel(extent):
    modes = jnp.arange(extent, dtype=jnp.int32)
    modes = jnp.where(2 * modes < extent, modes, modes - extent)
    wavenum = modes.astype(jnp.float32) * (2.0 * math.pi / extent)
    squares = wavenum * wavenum
    norm_sq = squares[:, None, None] + squares[None, :, None] + squares[None, None, :]
    bounded = jnp.where(norm_sq > 0, norm_sq, 1.0)
    screened = jnp.where(
        norm_sq > 0,
        4.0 * math.pi / bounded * (1.0 - jnp.exp(-bounded / (4.0 * OMEGA * OMEGA))),
        math.pi / (OMEGA * OMEGA),
    )
    return screened / extent**3


def screened_potential(values, table, kernel):
    patterns = ("ga,abc->gbc", "gb,abc->agc", "gc,abc->abg")
    for pattern in patterns:
        values = jnp.einsum(pattern, table, values, preferred_element_type=jnp.float32).astype(
            jnp.bfloat16
        )
    values = (values.astype(jnp.float32) * kernel).astype(jnp.bfloat16)
    for ordinal, pattern in enumerate(patterns):
        values = jnp.einsum(pattern, table, values, preferred_element_type=jnp.float32)
        if ordinal < 2:
            values = values.astype(jnp.bfloat16)
    return values


def greet(count, me):
    barrier = pltpu.get_barrier_semaphore()

    @pl.loop(1, count)
    def _(step):
        peer = lax.rem(me + step, count)
        pl.semaphore_signal(barrier, inc=1, device_id={"band": peer}, device_id_type=MESH)

    pl.semaphore_wait(barrier, count - 1)


def slabs_body(count, arrays, *refs):
    ins, outs = refs[:arrays], refs[arrays : 2 * arrays]
    send_sem, recv_sem, own_sem = refs[2 * arrays :]
    me = lax.axis_index("band")
    greet(count, me)

    def remote(which, peer, slot):
        return pltpu.make_async_remote_copy(
            src_ref=ins[which].at[peer],
            dst_ref=outs[which].at[slot],
            send_sem=send_sem.at[which, peer],
            recv_sem=recv_sem.at[which, slot],
            device_id={"band": peer},
            device_id_type=MESH,
        )

    def own(which):
        return pltpu.make_async_copy(ins[which].at[me], outs[which].at[me], own_sem.at[which])

    for which in range(arrays):

        @pl.loop(1, count)
        def _(step):
            remote(which, lax.rem(me + step, count), me).start()

        own(which).start()
    for which in range(arrays):
        own(which).wait()

        @pl.loop(1, count)
        def _(step):
            remote(which, lax.rem(me + step, count), me).wait_send()

        @pl.loop(1, count)
        def _(step):
            peer = lax.rem(me + count - step, count)
            remote(which, peer, peer).wait_recv()


def to_slabs(arrays, collective_id):
    count = lax.axis_size("band")
    number = len(arrays)
    shape = arrays[0].shape
    size = math.prod(shape)
    return pl.pallas_call(
        functools.partial(slabs_body, count, number),
        out_shape=[jax.ShapeDtypeStruct(shape, a.dtype) for a in arrays],
        in_specs=[pl.BlockSpec(memory_space=pltpu.VMEM)] * number,
        out_specs=[pl.BlockSpec(memory_space=pltpu.VMEM)] * number,
        scratch_shapes=[
            pltpu.SemaphoreType.DMA((number, count)),
            pltpu.SemaphoreType.DMA((number, count)),
            pltpu.SemaphoreType.DMA((number,)),
        ],
        cost_estimate=pl.CostEstimate(
            flops=0, bytes_accessed=size * 40 * number, transcendentals=0
        ),
        compiler_params=pltpu.CompilerParams(
            collective_id=collective_id, has_side_effects=True
        ),
        name="to_slabs",
    )(*arrays)


def summed_body(count, part_ref, total_ref, parts, send_sem, recv_sem):
    me = lax.axis_index("band")
    greet(count, me)

    def remote(peer, slot):
        return pltpu.make_async_remote_copy(
            src_ref=part_ref,
            dst_ref=parts.at[slot],
            send_sem=send_sem.at[peer],
            recv_sem=recv_sem.at[slot],
            device_id={"band": peer},
            device_id_type=MESH,
        )

    @pl.loop(1, count)
    def _(step):
        remote(lax.rem(me + step, count), me).start()

    parts[pl.ds(me, 1)] = part_ref[...][None]

    @pl.loop(1, count)
    def _(step):
        remote(lax.rem(me + step, count), me).wait_send()

    @pl.loop(1, count)
    def _(step):
        peer = lax.rem(me + count - step, count)
        remote(peer, peer).wait_recv()

    total_ref[...] = jnp.sum(parts[...], axis=0)


def summed(part, collective_id):
    count = lax.axis_size("band")
    return pl.pallas_call(
        functools.partial(summed_body, count),
        out_shape=jax.ShapeDtypeStruct(part.shape, part.dtype),
        in_specs=[pl.BlockSpec(memory_space=pltpu.VMEM)],
        out_specs=pl.BlockSpec(memory_space=pltpu.VMEM),
        scratch_shapes=[
            pltpu.VMEM((count,) + part.shape, part.dtype),
            pltpu.SemaphoreType.DMA((count,)),
            pltpu.SemaphoreType.DMA((count,)),
        ],
        compiler_params=pltpu.CompilerParams(
            collective_id=collective_id, has_side_effects=True
        ),
        name="summed",
    )(part)


def rows_body(chunk, *refs):
    half = len(refs) // 2
    for line, rows in zip(refs[:half], refs[half:]):

        @pl.loop(0, line.shape[1] // chunk, unroll=4)
        def _(step):
            cut = pl.ds(pl.multiple_of(step * chunk, chunk), chunk)
            out = pl.ds(pl.multiple_of(step * (chunk // 128), chunk // 128), chunk // 128)
            wide = line[:, cut].astype(jnp.float32).reshape(chunk // 128, 128)
            rows[out, :] = wide.astype(rows.dtype)


def as_rows(*lines):
    number = len(lines)
    cells = lines[0].shape[1]
    return pl.pallas_call(
        functools.partial(rows_body, CHUNK),
        out_shape=[jax.ShapeDtypeStruct((cells // 128, 128), a.dtype) for a in lines],
        in_specs=[pl.BlockSpec(memory_space=pltpu.VMEM)] * number,
        out_specs=[pl.BlockSpec(memory_space=pltpu.VMEM)] * number,
        cost_estimate=pl.CostEstimate(
            flops=0, bytes_accessed=cells * 16 * number, transcendentals=0
        ),
        name="as_rows",
    )(*lines)


def local(orbitals, trial, occupations):
    count = lax.axis_size("band")
    cells = orbitals.shape[1]
    extent = NG
    table = cas_table(extent)
    kernel = lax.optimization_barrier(screened_kernel(extent))
    cube = (extent, extent, extent)
    fill = occupations.astype(jnp.bfloat16)

    (lined,) = as_rows(orbitals)
    (trial_rows,) = as_rows(trial)
    visitor, visitor_fill = passed_along((lined, fill), "band", 1)
    slab = (count, cells // count // 128, 128)
    grid_trial = lax.all_to_all(
        trial_rows.reshape(slab), "band", split_axis=0, concat_axis=0, tiled=True
    )
    own = lined.reshape(cube).astype(jnp.float32)
    own_weighted = own * fill[0].astype(jnp.float32)
    own_potential = screened_potential((own * own).astype(jnp.bfloat16), table, kernel)
    accumulated = own_potential * own_weighted

    other = visitor.reshape(cube).astype(jnp.float32)
    potential = screened_potential((own * other).astype(jnp.bfloat16), table, kernel)
    carried = passed_along((potential * own_weighted).astype(jnp.bfloat16), "band", -1)
    accumulated = accumulated + potential * (other * visitor_fill[0].astype(jnp.float32))
    accumulated = accumulated + carried.astype(jnp.float32)
    exchange = (-FRACTION * accumulated).astype(jnp.bfloat16).reshape(1, cells)

    (grid_exchange,) = to_slabs((exchange.reshape(slab),), 1)
    grid_exchange = grid_exchange.reshape(count, -1)
    grid_trial = grid_trial.reshape(count, -1)
    part = lax.dot_general(
        grid_exchange, grid_trial, (((1,), (1,)), ((), ())), preferred_element_type=jnp.float32
    )
    intersection_low = (summed(part, 2) / math.sqrt(cells)).astype(jnp.bfloat16)
    projected = -(
        lax.dot_general(
            intersection_low,
            grid_exchange,
            (((0,), (0,)), ((), ())),
            preferred_element_type=jnp.float32,
        )
        / math.sqrt(count)
    )
    return (exchange, projected.astype(jnp.bfloat16))


def solution(mesh):
    return jax.shard_map(
        local,
        mesh=mesh,
        in_specs=(P(("spin", "band"), None), P(("spin", "band"), None), P(("spin", "band"))),
        out_specs=(P(("spin", "band"), None), P("spin", "band")),
        check_vma=False,
    )
```

```python
import functools
import math

import jax
import jax.numpy as jnp
from jax import lax
from jax.experimental import pallas as pl
from jax.experimental.pallas import tpu as pltpu
from jax.sharding import PartitionSpec as P

NG = 64
FRACTION = 0.25
OMEGA = 1.0
CHUNK = 2048
TAG = 16
MESH = pl.DeviceIdType.MESH


def passed_along(value, axis, steps):
    count = lax.axis_size(axis)
    pairs = [(source, (source + steps) % count) for source in range(count)]
    return lax.ppermute(value, axis, pairs)


def cas_table(extent):
    indices = jnp.arange(extent, dtype=jnp.int32)
    products = indices[:, None] * indices[None, :] % extent
    phases = products.astype(jnp.float32) * (2.0 * math.pi / extent)
    return (jnp.cos(phases) + jnp.sin(phases)).astype(jnp.bfloat16)


def screened_kernel(extent):
    modes = jnp.arange(extent, dtype=jnp.int32)
    modes = jnp.where(2 * modes < extent, modes, modes - extent)
    wavenum = modes.astype(jnp.float32) * (2.0 * math.pi / extent)
    squares = wavenum * wavenum
    norm_sq = squares[:, None, None] + squares[None, :, None] + squares[None, None, :]
    bounded = jnp.where(norm_sq > 0, norm_sq, 1.0)
    screened = jnp.where(
        norm_sq > 0,
        4.0 * math.pi / bounded * (1.0 - jnp.exp(-bounded / (4.0 * OMEGA * OMEGA))),
        math.pi / (OMEGA * OMEGA),
    )
    return screened / extent**3


def screened_potential(values, table, kernel):
    patterns = ("ga,abc->gbc", "gb,abc->agc", "gc,abc->abg")
    for pattern in patterns:
        values = jnp.einsum(pattern, table, values, preferred_element_type=jnp.float32).astype(
            jnp.bfloat16
        )
    values = (values.astype(jnp.float32) * kernel).astype(jnp.bfloat16)
    for ordinal, pattern in enumerate(patterns):
        values = jnp.einsum(pattern, table, values, preferred_element_type=jnp.float32)
        if ordinal < 2:
            values = values.astype(jnp.bfloat16)
    return values


def greet(count, me):
    barrier = pltpu.get_barrier_semaphore()

    @pl.loop(1, count)
    def _(step):
        peer = lax.rem(me + step, count)
        pl.semaphore_signal(barrier, inc=1, device_id={"band": peer}, device_id_type=MESH)

    pl.semaphore_wait(barrier, count - 1)


def slabs_body(count, arrays, *refs):
    ins, outs = refs[:arrays], refs[arrays : 2 * arrays]
    send_sem, recv_sem, own_sem = refs[2 * arrays :]
    me = lax.axis_index("band")
    greet(count, me)

    def remote(which, peer, slot):
        return pltpu.make_async_remote_copy(
            src_ref=ins[which].at[peer],
            dst_ref=outs[which].at[slot],
            send_sem=send_sem.at[which, peer],
            recv_sem=recv_sem.at[which, slot],
            device_id={"band": peer},
            device_id_type=MESH,
        )

    def own(which):
        return pltpu.make_async_copy(ins[which].at[me], outs[which].at[me], own_sem.at[which])

    for which in range(arrays):

        @pl.loop(1, count)
        def _(step):
            remote(which, lax.rem(me + step, count), me).start()

        own(which).start()
    for which in range(arrays):
        own(which).wait()

        @pl.loop(1, count)
        def _(step):
            remote(which, lax.rem(me + step, count), me).wait_send()

        @pl.loop(1, count)
        def _(step):
            peer = lax.rem(me + count - step, count)
            remote(which, peer, peer).wait_recv()


def to_slabs(arrays, collective_id):
    count = lax.axis_size("band")
    number = len(arrays)
    shape = arrays[0].shape
    size = math.prod(shape)
    return pl.pallas_call(
        functools.partial(slabs_body, count, number),
        out_shape=[jax.ShapeDtypeStruct(shape, a.dtype) for a in arrays],
        in_specs=[pl.BlockSpec(memory_space=pltpu.VMEM)] * number,
        out_specs=[pl.BlockSpec(memory_space=pltpu.VMEM)] * number,
        scratch_shapes=[
            pltpu.SemaphoreType.DMA((number, count)),
            pltpu.SemaphoreType.DMA((number, count)),
            pltpu.SemaphoreType.DMA((number,)),
        ],
        cost_estimate=pl.CostEstimate(
            flops=0, bytes_accessed=size * 40 * number, transcendentals=0
        ),
        compiler_params=pltpu.CompilerParams(
            collective_id=collective_id, has_side_effects=True
        ),
        name="to_slabs",
    )(*arrays)


def summed_body(count, part_ref, total_ref, parts, send_sem, recv_sem):
    me = lax.axis_index("band")
    greet(count, me)

    def remote(peer, slot):
        return pltpu.make_async_remote_copy(
            src_ref=part_ref,
            dst_ref=parts.at[slot],
            send_sem=send_sem.at[peer],
            recv_sem=recv_sem.at[slot],
            device_id={"band": peer},
            device_id_type=MESH,
        )

    @pl.loop(1, count)
    def _(step):
        remote(lax.rem(me + step, count), me).start()

    parts[pl.ds(me, 1)] = part_ref[...][None]

    @pl.loop(1, count)
    def _(step):
        remote(lax.rem(me + step, count), me).wait_send()

    @pl.loop(1, count)
    def _(step):
        peer = lax.rem(me + count - step, count)
        remote(peer, peer).wait_recv()

    total_ref[...] = jnp.sum(parts[...], axis=0)


def summed(part, collective_id):
    count = lax.axis_size("band")
    return pl.pallas_call(
        functools.partial(summed_body, count),
        out_shape=jax.ShapeDtypeStruct(part.shape, part.dtype),
        in_specs=[pl.BlockSpec(memory_space=pltpu.VMEM)],
        out_specs=pl.BlockSpec(memory_space=pltpu.VMEM),
        scratch_shapes=[
            pltpu.VMEM((count,) + part.shape, part.dtype),
            pltpu.SemaphoreType.DMA((count,)),
            pltpu.SemaphoreType.DMA((count,)),
        ],
        compiler_params=pltpu.CompilerParams(
            collective_id=collective_id, has_side_effects=True
        ),
        name="summed",
    )(part)


def rows_body(chunk, *refs):
    half = len(refs) // 2
    for line, rows in zip(refs[:half], refs[half:]):

        @pl.loop(0, line.shape[1] // chunk, unroll=4)
        def _(step):
            cut = pl.ds(pl.multiple_of(step * chunk, chunk), chunk)
            out = pl.ds(pl.multiple_of(step * (chunk // 128), chunk // 128), chunk // 128)
            wide = line[:, cut].astype(jnp.float32).reshape(chunk // 128, 128)
            rows[out, :] = wide.astype(rows.dtype)


def tagged_body(chunk, line, tag, rows):
    rows_body(chunk, line, rows)
    full = line.shape[1] // 128
    rows[full:, :] = jnp.broadcast_to(tag[...], (TAG, 128)).astype(rows.dtype)


def tagged_rows(line, tag):
    cells = line.shape[1]
    return pl.pallas_call(
        functools.partial(tagged_body, CHUNK),
        out_shape=jax.ShapeDtypeStruct((cells // 128 + TAG, 128), line.dtype),
        in_specs=[pl.BlockSpec(memory_space=pltpu.VMEM)] * 2,
        out_specs=pl.BlockSpec(memory_space=pltpu.VMEM),
        name="tagged_rows",
    )(line, tag)


def as_rows(*lines):
    number = len(lines)
    cells = lines[0].shape[1]
    return pl.pallas_call(
        functools.partial(rows_body, CHUNK),
        out_shape=[jax.ShapeDtypeStruct((cells // 128, 128), a.dtype) for a in lines],
        in_specs=[pl.BlockSpec(memory_space=pltpu.VMEM)] * number,
        out_specs=[pl.BlockSpec(memory_space=pltpu.VMEM)] * number,
        cost_estimate=pl.CostEstimate(
            flops=0, bytes_accessed=cells * 16 * number, transcendentals=0
        ),
        name="as_rows",
    )(*lines)


def local(orbitals, trial, occupations):
    count = lax.axis_size("band")
    cells = orbitals.shape[1]
    extent = NG
    table = cas_table(extent)
    kernel = screened_kernel(extent)
    cube = (extent, extent, extent)
    fill = occupations.astype(jnp.bfloat16)

    tag = jnp.broadcast_to(occupations.astype(jnp.float32).reshape(1, 1), (1, 128))
    lined = tagged_rows(orbitals, tag)
    (trial_rows,) = as_rows(trial)
    passed = passed_along(lined, "band", 1)
    full = cells // 128
    visitor, visitor_fill = passed[:full], passed[full, :1]
    own = lined[:full].reshape(cube).astype(jnp.float32)
    own_weighted = own * fill[0].astype(jnp.float32)
    own_potential = screened_potential((own * own).astype(jnp.bfloat16), table, kernel)
    accumulated = own_potential * own_weighted

    other = visitor.reshape(cube).astype(jnp.float32)
    potential = screened_potential((own * other).astype(jnp.bfloat16), table, kernel)
    carried = passed_along((potential * own_weighted).astype(jnp.bfloat16), "band", -1)
    accumulated = accumulated + potential * (other * visitor_fill[0].astype(jnp.float32))
    accumulated = accumulated + carried.astype(jnp.float32)
    exchange = (-FRACTION * accumulated).astype(jnp.bfloat16).reshape(1, cells)

    slab = (count, cells // count // 128, 128)
    grid_exchange, grid_trial = to_slabs((exchange.reshape(slab), trial_rows.reshape(slab)), 1)
    grid_exchange = grid_exchange.reshape(count, -1)
    grid_trial = grid_trial.reshape(count, -1)
    part = lax.dot_general(
        grid_exchange, grid_trial, (((1,), (1,)), ((), ())), preferred_element_type=jnp.float32
    )
    intersection_low = (summed(part, 2) / math.sqrt(cells)).astype(jnp.bfloat16)
    projected = -(
        lax.dot_general(
            intersection_low,
            grid_exchange,
            (((0,), (0,)), ((), ())),
            preferred_element_type=jnp.float32,
        )
        / math.sqrt(count)
    )
    return (exchange, projected.astype(jnp.bfloat16))


def solution(mesh):
    return jax.shard_map(
        local,
        mesh=mesh,
        in_specs=(P(("spin", "band"), None), P(("spin", "band"), None), P(("spin", "band"))),
        out_specs=(P(("spin", "band"), None), P("spin", "band")),
        check_vma=False,
    )
```
